128 devices in a mesh: grp: 2 (over core), dev: 64 (over x, z, y).
Axes of the slice: x: 4, y: 4, z: 4, core: 2. Of those that a mesh axis runs over, the one named last changes fastest.
Arguments:
- state: float32 [2, 24, 24, 16384], P(None, None, None, ('grp', 'dev')), may hold values from -6 to 6
- hamiltonian: float32 [24, 24], replicated, may hold values from -1.2 to 1.2
- mode_rates: float32 [96], replicated, may hold values from 0.05 to 2
- ado_modes: int32 [3, 16384], P(None, ('grp', 'dev')), may hold values from 0 to 96
- link_src: int32 [8, 16384], P(None, ('grp', 'dev')), may hold values from 0 to 383, as said below
- link_site: int32 [8, 16384], P(None, ('grp', 'dev')), may hold values from 0 to 23
- link_coef: float32 [4, 8, 16384], P(None, None, ('grp', 'dev')), may hold values from -2.4 to 2.4
- send_ids: int32 [128, 256], P(('grp', 'dev')), may hold values from 0 to 127
- step_units: int32 [], replicated, may hold values from 12 to 16
Outputs:
- new_state: float32 [2, 24, 24, 16384], P(None, None, None, ('grp', 'dev'))
- error_norm: float32 [], replicated
The draws below stay inside these ranges and needn't reach their ends.
Inputs may be any that keep to these rules, and one draw needn't show every extreme that they name: `link_src`: on each device every received position 128 to 383 is named by 1 to 4 couplings of that device's matrices, and some position by exactly 4.
All inputs are finite; a program needn't handle non-finite values.
Results may differ from the reference program's by a relative error of at most 0.0003.
Values sent between devices are 32-bit elements; how exact they have to be, the bound alone decides.
No kernel may reach another device: no remote copies, remote signals or barrier semaphores. Data moves between devices by JAX's collectives and lax.ppermute only.
A program may use at most 128 MiB of HBM per device.

```python
import math
import jax
import jax.numpy as jnp
from jax import lax

N = 24
MODES = 96
DEPTH = 3
LINKS = 8
SLOT = 2
USES = 4
ADO_DEV = 128
PEERS = 128
ADOS = 16384
RECV = 256


def draw_link_src(key, part):

    def one_device(device_key):
        key_rank, key_local, key_keep, key_full = jax.random.split(device_key, 4)
        ranking = jax.random.permutation(key_rank, LINKS * ADO_DEV)
        local = jax.random.randint(key_local, (LINKS * ADO_DEV,), 0, ADO_DEV)
        keeping = jax.random.randint(key_keep, (LINKS * ADO_DEV,), 0, 2)
        fullest = jax.random.randint(key_full, (), 0, RECV)
        position = ranking % RECV
        copies = ranking // RECV
        remote = (ranking < RECV * USES) & ((copies == 0) | (keeping == 1) | (position == fullest))
        chosen = jnp.where(remote, ADO_DEV + position, local)
        return chosen.astype(jnp.int32).reshape(LINKS, ADO_DEV)
    blocks = jax.vmap(one_device)(jax.random.split(jax.random.fold_in(key, 7), PEERS))
    return jnp.transpose(blocks, (1, 0, 2)).reshape(LINKS, PEERS * ADO_DEV)


def set_ends(values, stream_key, least, high):
    index_at = [jax.random.randint(jax.random.fold_in(stream_key, axis), (), 0, length) for axis, length in enumerate(values.shape)]
    longest = values.shape.index(max(values.shape))
    neighbour = index_at[:longest] + [(index_at[longest] + 1) % values.shape[longest]] + index_at[longest + 1:]
    return values.at[tuple(index_at)].set(least).at[tuple(neighbour)].set(high)


def shard_levels(key, dims, cuts, smallest, high):
    def one(dim, shards_of):
        draws = jax.random.uniform(jax.random.fold_in(jax.random.fold_in(key, 6), dim), (shards_of,), jnp.float32, smallest / len(cuts), high / len(cuts))
        return jnp.repeat(jnp.exp(draws), dims[dim] // shards_of).reshape((-1,) + (1,) * (len(dims) - dim - 1))

    factor_of = one(*cuts[0])
    for cut in cuts[1:]:
        factor_of = factor_of * one(*cut)
    return factor_of


def normal_values(key, extent, scale, bound, cuts=(), kind=jnp.bfloat16):
    values = scale * jax.random.normal(key, extent, jnp.float32)
    if cuts:
        values = values * shard_levels(key, extent, cuts, -0.22, 0.18)
    return jnp.clip(values, -bound, bound).astype(kind)


def setup_inputs(seed: int = 0) -> dict:
    key_list = jax.random.split(jax.random.key(seed), 10)
    state = normal_values(key_list[0], (2, N, N, ADOS), 1.0, 6.0, ((3, 128),), jnp.float32)
    hamiltonian = normal_values(key_list[1], (N, N), 0.3, 1.2, (), jnp.float32)
    mode_rates = jnp.clip(jnp.exp(jax.random.uniform(key_list[2], (MODES,), jnp.float32, math.log(0.05), math.log(2.0))), 0.05, 2.0)
    ado_modes = set_ends(jax.random.randint(key_list[3], (DEPTH, ADOS), 0, MODES + 1), jax.random.fold_in(key_list[3], 1), 0, MODES).astype(jnp.int32)
    link_src = draw_link_src(jax.random.fold_in(key_list[9], 71), 0)
    link_site = set_ends(jax.random.randint(key_list[5], (LINKS, ADOS), 0, N), jax.random.fold_in(key_list[5], 1), 0, N - 1).astype(jnp.int32)
    link_coef = normal_values(key_list[6], (4, LINKS, ADOS), 0.8, 2.4, ((2, 128),), jnp.float32)
    send_ids = set_ends(jax.random.randint(key_list[7], (PEERS, RECV), 0, ADO_DEV), jax.random.fold_in(key_list[7], 1), 0, ADO_DEV - 1).astype(jnp.int32)
    step_units = jax.random.randint(key_list[8], (), 12, 17).astype(jnp.int32)
    return dict(state=state, hamiltonian=hamiltonian, mode_rates=mode_rates, ado_modes=ado_modes, link_src=link_src, link_site=link_site, link_coef=link_coef, send_ids=send_ids, step_units=step_units)


TABLEAU = ((0.2,), (3.0 / 40, 9.0 / 40), (44.0 / 45, -56.0 / 15, 32.0 / 9), (19372.0 / 6561, -25360.0 / 2187, 64448.0 / 6561, -212.0 / 729), (9017.0 / 3168, -355.0 / 33, 46732.0 / 5247, 49.0 / 176, -5103.0 / 18656), (35.0 / 384, 0.0, 500.0 / 1113, 125.0 / 192, -2187.0 / 6784, 11.0 / 84))
ERRORS = (71.0 / 57600, 0.0, -71.0 / 16695, 71.0 / 1920, -17253.0 / 339200, 22.0 / 525, -1.0 / 40)
ABS_TOL = 0.001
REL_TOL = 0.01
UNIT_STEP = 1.0 / 64

def commute(symmetric, current):
    left_prod = jnp.einsum('ab,sbcx->sacx', symmetric, current, precision=lax.Precision.HIGHEST)
    right_prod = jnp.einsum('sabx,bc->sacx', current, symmetric, precision=lax.Precision.HIGHEST)
    return left_prod - right_prod

def decay_rates(ado_modes, mode_rates):
    extended = jnp.concatenate([mode_rates, jnp.zeros((1,), mode_rates.dtype)])
    levels = jnp.arange(extended.shape[0], dtype=jnp.int32)
    hits = (ado_modes[:, None, :] == levels[None, :, None]).astype(mode_rates.dtype)
    return lax.optimization_barrier(jnp.sum(hits * extended[None, :, None], axis=(0, 1)))

def link_term(source, sites, coef):
    levels = jnp.arange(source.shape[1], dtype=jnp.int32)
    indicator = (levels[:, None] == sites[None, :]).astype(source.dtype)
    row_mask = indicator[:, None, :]
    column_mask = indicator[None, :, :]
    weight_real = coef[0] * row_mask - coef[2] * column_mask
    weight_imag = coef[1] * row_mask - coef[3] * column_mask
    real_part = weight_real * source[0] - weight_imag * source[1]
    imag_part = weight_real * source[1] + weight_imag * source[0]
    return jnp.stack([imag_part, -real_part])

def derivative(current, fetch, symmetric, decay, link_site, link_coef):
    commutator = commute(symmetric, current)
    total = jnp.stack([commutator[1], -commutator[0]]) - decay[None, None, None, :] * current
    for link in range(link_site.shape[0]):
        total = total + link_term(fetch(link), link_site[link], link_coef[:, link])
    return total

def dormand_prince(start, step_size, evaluate):
    sections = [evaluate(start)]
    inner = start
    for weights in TABLEAU:
        inner = start
        for weight, section in zip(weights, sections):
            if weight != 0.0:
                inner = inner + step_size * weight * section
        sections.append(evaluate(inner))
    error = jnp.zeros_like(start)
    for weight, section in zip(ERRORS, sections):
        if weight != 0.0:
            error = error + step_size * weight * section
    scale = ABS_TOL + REL_TOL * jnp.maximum(jnp.abs(start), jnp.abs(inner))
    partial_sum = jnp.sum(jnp.square(error / scale))
    return (inner, partial_sum)

def reference(state, hamiltonian, mode_rates, ado_modes, link_src, link_site, link_coef, send_ids, step_units):
    total_ados = state.shape[3]
    owner = jnp.arange(total_ados, dtype=jnp.int32) // ADO_DEV
    remote = jnp.maximum(link_src - ADO_DEV, 0)
    source_dev = remote // SLOT
    within = remote % SLOT
    column = owner[None, :] * SLOT + within
    sent = send_ids[source_dev, column]
    global_index = jnp.where(link_src < ADO_DEV, owner[None, :] * ADO_DEV + link_src, source_dev * ADO_DEV + sent).astype(jnp.int32)
    symmetric = 0.5 * (hamiltonian + hamiltonian.T)
    decay = decay_rates(ado_modes, mode_rates)
    step_size = step_units.astype(state.dtype) * UNIT_STEP

    def evaluate(current):
        return derivative(current, lambda link: jnp.take(current, global_index[link], axis=3), symmetric, decay, link_site, link_coef)
    new_state, partial_sum = dormand_prince(state, step_size, evaluate)
    entries = 2 * state.shape[1] * state.shape[2] * total_ados
    return (new_state, jnp.sqrt(partial_sum / entries))
```

```python
from fractions import Fraction

import jax
import jax.numpy as jnp
from jax import lax
from jax.experimental import pallas as pl
from jax.experimental.pallas import tpu as pltpu
from jax.sharding import PartitionSpec as P

ALL = ("grp", "dev")

TABLEAU = (
    ("1/5",),
    ("3/40", "9/40"),
    ("44/45", "-56/15", "32/9"),
    ("19372/6561", "-25360/2187", "64448/6561", "-212/729"),
    ("9017/3168", "-355/33", "46732/5247", "49/176", "-5103/18656"),
    ("35/384", "0", "500/1113", "125/192", "-2187/6784", "11/84"),
)
ERRORS = ("71/57600", "0", "-71/16695", "71/1920", "-17253/339200", "22/525", "-1/40")
ABS_TOL = 0.001
REL_TOL = 0.01
UNIT_STEP = 1.0 / 64

N = 24
LINKS = 8
SLOT = 2
USES = 4
LANES = 128
SQ = N * N
ROWS = 2 * SQ
LINE = 4 * N
PIECES = SLOT * USES
FEATURES = PIECES * LINE
BLOCKS = FEATURES // LANES
COUPLINGS = LINKS * LANES
HIGHEST = lax.Precision.HIGHEST
F32 = jnp.float32
BF16 = jnp.bfloat16


def step_polynomials():
    def axpy(left, weight, right):
        size = max(len(left), len(right))
        left = left + [Fraction(0)] * (size - len(left))
        right = right + [Fraction(0)] * (size - len(right))
        return [a + weight * b for a, b in zip(left, right)]

    inner = [Fraction(1)]
    sections = [[Fraction(0)] + inner]
    for weights in TABLEAU:
        inner = [Fraction(1)]
        for weight, section in zip(weights, sections):
            inner = axpy(inner, Fraction(weight), section)
        sections.append([Fraction(0)] + inner)
    error = [Fraction(0)]
    for weight, section in zip(ERRORS, sections):
        error = axpy(error, Fraction(weight), section)
    return [float(x) for x in inner], [float(x) for x in error]


NEW, ERR = step_polynomials()
POWERS = len(ERR) - 1


def split(x):
    high = x.astype(BF16)
    low = (x - high.astype(F32)).astype(BF16)
    return high, low


def dot(a, b, **kw):
    return jnp.dot(a, b, preferred_element_type=F32, **kw)


def div24(x):
    return lax.shift_right_logical(x * 2731, 16)


def call(body, outs, scratch=(), flops=1000000, name=None, smem=(), args=()):
    specs = [
        pl.BlockSpec(memory_space=pltpu.SMEM if i in smem else pltpu.VMEM) for i in range(len(args))
    ]
    return pl.pallas_call(
        body,
        out_shape=[jax.ShapeDtypeStruct(s, d) for s, d in outs],
        in_specs=specs,
        out_specs=[pl.BlockSpec(memory_space=pltpu.VMEM) for _ in outs],
        scratch_shapes=[pltpu.VMEM(s, d) for s, d in scratch],
        compiler_params=pltpu.CompilerParams(vmem_limit_bytes=24 * 1024 * 1024),
        cost_estimate=pl.CostEstimate(flops=flops, bytes_accessed=4000000, transcendentals=0),
        name=name,
    )(*args)


def plan_body(src_ref, site_ref, place_ref, ask_ref):
    src = src_ref[...]
    srcf = src.astype(F32)
    turned = jnp.concatenate([srcf, jnp.zeros((LANES - LINKS, LANES), F32)], axis=0).T
    sub = lax.broadcasted_iota(jnp.int32, (LANES, LANES), 0)
    lane = lax.broadcasted_iota(jnp.int32, (LANES, LANES), 1)
    deep = lax.broadcasted_iota(jnp.int32, (COUPLINGS, LANES), 0)
    piece_row = lax.broadcasted_iota(jnp.int32, (PIECES, LANES), 0)
    asked = jnp.zeros((LANES, PIECES), F32)
    for l in range(LINKS):
        mine = jnp.broadcast_to(srcf[l : l + 1, :], (LANES, LANES))
        same = jnp.zeros((LANES, LANES), F32)
        for q in range(l + 1):
            other = jnp.broadcast_to(turned[:, q : q + 1], (LANES, LANES))
            hit = other == mine
            if q == l:
                hit = hit & (sub < lane)
            same = same + jnp.where(hit, 1.0, 0.0)
        rank = jnp.sum(same, axis=0, keepdims=True).astype(jnp.int32)
        place = src[l : l + 1, :] - LANES
        slot = lax.bitwise_and(place, SLOT - 1)
        owner = lax.shift_right_arithmetic(place, 1)
        index = jnp.where(place >= 0, (slot * USES + rank) * LANES + owner, -1)
        hot = jnp.where(deep == jnp.broadcast_to(index, (COUPLINGS, LANES)), 1.0, 0.0).astype(BF16)
        place_ref[:, l * LANES : (l + 1) * LANES] = hot
        owned = jnp.where(sub == owner, 1.0, 0.0).astype(BF16)
        wanted = jnp.where(
            (piece_row == slot * USES + rank) & (place >= 0), site_ref[l : l + 1, :].astype(F32), 0.0
        ).astype(BF16)
        asked = asked + lax.dot_general(
            owned, wanted, (((1,), (1,)), ((), ())), preferred_element_type=F32
        )
    ask_ref[...] = jnp.zeros((LANES, LANES), F32)
    ask_ref[:, 0:PIECES] = asked


def tables_body(
    units_ref, ham_ref, rates_ref, modes_ref, src_ref, coef_ref, send_ref,
    high_ref, low_ref, decay_ref, own_ref, pick_ref, scaled_ref,
):
    h = units_ref[0].astype(F32) * UNIT_STEP
    ham = ham_ref[...]
    row = lax.broadcasted_iota(jnp.int32, (N, N), 0)
    column = lax.broadcasted_iota(jnp.int32, (N, N), 1)
    unit = jnp.where(row == column, 1.0, 0.0)
    flipped = lax.dot_general(
        unit, ham, (((1,), (1,)), ((), ())), precision=HIGHEST, preferred_element_type=F32
    )
    sym = h * (0.5 * (ham + flipped))
    at = lax.broadcasted_iota(jnp.int32, (N, SQ), 1)
    row = lax.broadcasted_iota(jnp.int32, (N, SQ), 0)
    first = div24(at)
    same_second = row == at - first * N
    by_first = dot(sym, jnp.where(row == first, 1.0, 0.0), precision=HIGHEST)
    by_second = dot(sym, jnp.where(same_second, 1.0, 0.0), precision=HIGHEST)
    for a in range(N):
        block = jnp.where(same_second, jnp.broadcast_to(by_first[a : a + 1, :], (N, SQ)), 0.0)
        high, low = split(block - jnp.where(first == a, by_second, 0.0))
        high_ref[a * N : (a + 1) * N, :] = high
        low_ref[a * N : (a + 1) * N, :] = low
    level = lax.broadcasted_iota(jnp.int32, (rates_ref.shape[1], LANES), 0)
    hits = jnp.zeros((rates_ref.shape[1], LANES), F32)
    for m in range(modes_ref.shape[0]):
        hits = hits + jnp.where(level == modes_ref[m : m + 1, :], 1.0, 0.0)
    rates = jnp.broadcast_to(rates_ref[...], (8, rates_ref.shape[1]))
    decay_ref[...] = h * dot(rates, hits, precision=HIGHEST)
    sub = lax.broadcasted_iota(jnp.int32, (LANES, LANES), 0)
    for l in range(LINKS):
        hot = jnp.where(sub == src_ref[l : l + 1, :], 1.0, 0.0).astype(BF16)
        own_ref[l, 0:LANES, :] = hot
        own_ref[l, LANES : 2 * LANES, :] = hot
    wide = SLOT * LANES
    i = lax.broadcasted_iota(jnp.int32, (wide, wide), 0)
    p = lax.broadcasted_iota(jnp.int32, (wide, wide), 1)
    order = jnp.where(
        i == lax.bitwise_and(p, LANES - 1) * SLOT + lax.shift_right_logical(p, 7), 1.0, 0.0
    ).astype(BF16)
    ids = jnp.broadcast_to(send_ref[...].astype(F32), (8, wide)).astype(BF16)
    sorted_ids = dot(ids, order)[0:1, :].astype(jnp.int32)
    sub = lax.broadcasted_iota(jnp.int32, (LANES, wide), 0)
    hot = jnp.where(sub == sorted_ids, 1.0, 0.0).astype(BF16)
    pick_ref[0:LANES, :] = hot
    pick_ref[LANES : 2 * LANES, :] = hot
    scaled_ref[...] = h * coef_ref[...]


def lines(read_row, read_column, sites, store):
    for kind, read in ((0, read_row), (1, read_column)):
        kept = [[[None] * 3 for _ in range(2)] for _ in sites]
        for k in range(N):
            tile = [[read(c, k, t) for t in range(3)] for c in range(2)]
            for u, site in enumerate(sites):
                hit = site == k if k else None
                for c in range(2):
                    for t in range(3):
                        kept[u][c][t] = (
                            jnp.where(hit, tile[c][t], kept[u][c][t]) if k else tile[c][t]
                        )
        for u in range(len(sites)):
            for c in range(2):
                for t in range(3):
                    store(u, kind * 2 * N + c * N + t * 8, kept[u][c][t])


def local_part(v_ref, high_ref, low_ref, decay_ref, own_ref, site_ref, base, line, both_ref, even, odd):
    real, imag = v_ref[0:SQ, :], v_ref[SQ:ROWS, :]
    real_high, real_low = split(real)
    imag_high, imag_low = split(imag)
    high = jnp.concatenate([real_high, imag_high], axis=0)
    low = jnp.concatenate([real_low, imag_low], axis=0)
    both_ref[...] = jnp.concatenate([high, low], axis=1)

    def fetch(l, place):
        place[...] = dot(both_ref[...], own_ref[l])

    def pick(l, place):
        site = jnp.broadcast_to(site_ref[pl.ds(l, 1), :], (8, LANES))

        def store(u, f, value):
            line[l, f : f + 8, :] = value

        lines(
            lambda c, k, t: place[pl.ds(c * SQ + k * N + t * 8, 8), :],
            lambda c, k, t: place[pl.ds(c * SQ + t * 8 * N + k, 8, stride=N), :],
            [site],
            store,
        )

    def pair(i, carry):
        fetch(2 * i + 1, odd)
        pick(2 * i, even)
        fetch(jnp.minimum(2 * i + 2, LINKS - 1), even)
        pick(2 * i + 1, odd)
        return carry

    fetch(0, even)
    lax.fori_loop(0, LINKS // 2, pair, 0)
    x_high = jnp.concatenate([real_high, imag_high], axis=1)
    x_low = jnp.concatenate([real_low, imag_low], axis=1)
    turned = dot(high_ref[...], x_high) + dot(high_ref[...], x_low) + dot(low_ref[...], x_high)
    decay = jnp.broadcast_to(decay_ref[0:1, :], (SQ, LANES))
    base[0:SQ, :] = turned[:, LANES:] - decay * real
    base[SQ:ROWS, :] = -turned[:, :LANES] - decay * imag


def pack_part(v_ref, pick_ref, sites, send_ref, full, feats):
    high, low = split(v_ref[...])
    picked = dot(jnp.concatenate([high, low], axis=1), pick_ref[...])
    for s in range(SLOT):
        full[s] = picked[:, s * LANES : (s + 1) * LANES]
    for s in range(SLOT):
        wanted = [
            jnp.broadcast_to(sites[s * USES + u : s * USES + u + 1, :], (8, LANES))
            for u in range(USES)
        ]

        def store(u, f, value):
            row = (s * USES + u) * LINE + f
            feats[row : row + 8, :] = value

        lines(
            lambda c, k, t: full[s, pl.ds(c * SQ + k * N + t * 8, 8), :],
            lambda c, k, t: full[s, pl.ds(c * SQ + t * 8 * N + k, 8, stride=N), :],
            wanted,
            store,
        )
    for k in range(BLOCKS):
        send_ref[pl.ds(k, LANES, stride=BLOCKS), :] = feats[k * LANES : (k + 1) * LANES, :].T


def first_pack(v, pick, asked):
    def body(v_ref, pick_ref, asked_ref, send_ref, want_ref, full, feats):
        want = asked_ref[...].T[0:PIECES, :].astype(jnp.int32)
        want_ref[...] = want
        pack_part(v_ref, pick_ref, want, send_ref, full, feats)

    return call(
        body,
        [((BLOCKS * LANES, LANES), F32), ((PIECES, LANES), jnp.int32)],
        [((SLOT, ROWS, LANES), F32), ((FEATURES, LANES), F32)],
        flops=10**8, name="pack_first", args=(v, pick, asked),
    )


def gather_part(got_ref, place_ref, site_ref, coef_ref, base_ref, line_ref, emit, feats, cols):
    for k in range(BLOCKS):
        feats[k * LANES : (k + 1) * LANES, :] = got_ref[pl.ds(k, LANES, stride=BLOCKS), :].T
    wide = jnp.concatenate([feats[p * LINE : (p + 1) * LINE, :] for p in range(PIECES)], axis=1)
    high, low = split(wide)
    both = dot(jnp.concatenate([high, low], axis=0), place_ref[...])
    found = both[0:LINE, :] + both[LINE:, :]
    sites = [jnp.broadcast_to(site_ref[l : l + 1, :], (8, LANES)) for l in range(LINKS)]

    def term(kind, c, l):
        rows = slice(kind * 2 * N, (kind + 1) * 2 * N)
        x = found[rows, l * LANES : (l + 1) * LANES] + line_ref[l, rows, :]
        re, im = x[0:N], x[N:]
        row = 2 * kind * LINKS + l
        cr = jnp.broadcast_to(coef_ref[row : row + 1, :], (N, LANES))
        ci = jnp.broadcast_to(coef_ref[row + LINKS : row + LINKS + 1, :], (N, LANES))
        value = cr * im + ci * re if c == 0 else ci * im - cr * re
        return -value if kind else value

    for kind in (1, 0):
        for c in range(2):
            terms = [term(kind, c, l) for l in range(LINKS)]
            for k in range(N):
                hits = [site == k for site in sites]
                for t in range(3):
                    if kind:
                        total = jnp.zeros((8, LANES), F32)
                    else:
                        at = c * SQ + k * N + t * 8
                        total = base_ref[at : at + 8, :]
                        total = total + cols[pl.ds(c * SQ + t * 8 * N + k, 8, stride=N), :]
                    for l in range(LINKS):
                        total = total + jnp.where(hits[l], terms[l][t * 8 : t * 8 + 8], 0.0)
                    if kind:
                        at = c * SQ + k * N + t * 8
                        cols[at : at + 8, :] = total
                    else:
                        emit(at, total)


SCRATCH = [
    ((ROWS, LANES), F32),
    ((LINKS, LINE, LANES), F32),
    ((ROWS, 2 * LANES), BF16),
    ((SLOT, ROWS, LANES), F32),
    ((FEATURES, LANES), F32),
    ((ROWS, LANES), F32),
]


def advance(weight, got, v, total, tables, site, want):
    def body(got_ref, v_ref, total_ref, place_ref, high_ref, low_ref, decay_ref, own_ref, pick_ref,
             coef_ref, site_ref, want_ref, next_ref, send_ref, sum_ref, base, line, both, full, feats, cols):
        local_part(v_ref, high_ref, low_ref, decay_ref, own_ref, site_ref, base, line, both, full.at[0], full.at[1])

        def emit(at, value):
            next_ref[at : at + 8, :] = value
            sum_ref[at : at + 8, :] = total_ref[at : at + 8, :] + weight * value

        gather_part(got_ref, place_ref, site_ref, coef_ref, base, line, emit, feats, cols)
        pack_part(next_ref, pick_ref, want_ref[...], send_ref, full, feats)

    return call(
        body,
        [((ROWS, LANES), F32), ((BLOCKS * LANES, LANES), F32), ((ROWS, LANES), F32)],
        SCRATCH, name="advance", args=(got, v, total, *tables, site, want),
    )


def finish(got, v, before, state, new, tables, site):
    def body(got_ref, v_ref, before_ref, state_ref, new_ref, place_ref, high_ref, low_ref, decay_ref,
             own_ref, pick_ref, coef_ref, site_ref, out_ref, base, line, both, full, feats, cols, sums):
        local_part(v_ref, high_ref, low_ref, decay_ref, own_ref, site_ref, base, line, both, full.at[0], full.at[1])
        sums[...] = jnp.zeros((8, LANES), F32)

        def emit(at, value):
            rows = slice(at, at + 8)
            error = (
                ERR[POWERS - 2] * before_ref[rows, :]
                + ERR[POWERS - 1] * v_ref[rows, :]
                + ERR[POWERS] * value
            )
            largest = jnp.maximum(jnp.abs(state_ref[rows, :]), jnp.abs(new_ref[rows, :]))
            scaled = error / (ABS_TOL + REL_TOL * largest)
            sums[...] = sums[...] + scaled * scaled

        gather_part(got_ref, place_ref, site_ref, coef_ref, base, line, emit, feats, cols)
        out_ref[...] = jnp.broadcast_to(jnp.sum(sums[...], axis=0, keepdims=True), (LANES, LANES))

    (out,) = call(
        body,
        [((LANES, LANES), F32)],
        SCRATCH + [((8, LANES), F32)],
        name="finish", args=(got, v, before, state, new, *tables, site),
    )
    return out


def exchange(x):
    peers = LANES
    flat = x.reshape(peers, 1, x.size // peers)
    moved = lax.all_to_all(flat, ALL, split_axis=0, concat_axis=0, tiled=True)
    return moved.reshape(x.shape)


def shards(
    state, hamiltonian, mode_rates, ado_modes, link_src, link_site, link_coef, send_ids, step_units
):
    v = state.reshape(ROWS, LANES)
    place, ask = call(
        plan_body,
        [((COUPLINGS, COUPLINGS), BF16), ((LANES, LANES), F32)],
        flops=10**8, name="plan", args=(link_src, link_site),
    )
    asked = exchange(ask)
    high, low, decay, own, pick, coef = call(
        tables_body,
        [
            ((SQ, SQ), BF16),
            ((SQ, SQ), BF16),
            ((8, LANES), F32),
            ((LINKS, 2 * LANES, LANES), BF16),
            ((2 * LANES, SLOT * LANES), BF16),
            ((4 * LINKS, LANES), F32),
        ],
        flops=10**9, name="tables", smem=(0,),
        args=(
            step_units.reshape(1), hamiltonian, mode_rates.reshape(1, -1), ado_modes, link_src,
            link_coef.reshape(4 * LINKS, LANES), send_ids,
        ),
    )
    send, want = first_pack(v, pick, asked)
    total, before = v, v
    tables = (place, high, low, decay, own, pick, coef)
    for n in range(1, POWERS):
        before = v
        v, send, total = advance(NEW[n], exchange(send), before, total, tables, link_site, want)
    start = state.reshape(ROWS, LANES)
    sums = exchange(finish(exchange(send), v, before, start, total, tables, link_site))
    entries = state.size * lax.axis_size(ALL)
    return total.reshape(state.shape), jnp.sqrt(jnp.sum(sums) / entries)


def solution(mesh):
    return jax.shard_map(
        shards,
        mesh=mesh,
        in_specs=(
            P(None, None, None, ALL),
            P(),
            P(),
            P(None, ALL),
            P(None, ALL),
            P(None, ALL),
            P(None, None, ALL),
            P(ALL, None),
            P(),
        ),
        out_specs=(P(None, None, None, ALL), P()),
        check_vma=False,
    )
```

```python
from fractions import Fraction

import jax
import jax.numpy as jnp
from jax import lax
from jax.experimental import pallas as pl
from jax.experimental.pallas import tpu as pltpu
from jax.sharding import PartitionSpec as P

ALL = ("grp", "dev")

TABLEAU = (
    ("1/5",),
    ("3/40", "9/40"),
    ("44/45", "-56/15", "32/9"),
    ("19372/6561", "-25360/2187", "64448/6561", "-212/729"),
    ("9017/3168", "-355/33", "46732/5247", "49/176", "-5103/18656"),
    ("35/384", "0", "500/1113", "125/192", "-2187/6784", "11/84"),
)
ERRORS = ("71/57600", "0", "-71/16695", "71/1920", "-17253/339200", "22/525", "-1/40")
ABS_TOL = 0.001
REL_TOL = 0.01
UNIT_STEP = 1.0 / 64

N = 24
LINKS = 8
SLOT = 2
USES = 4
LANES = 128
SQ = N * N
ROWS = 2 * SQ
LINE = 4 * N
PIECES = SLOT * USES
FEATURES = PIECES * LINE
BLOCKS = FEATURES // LANES
COUPLINGS = LINKS * LANES
HIGHEST = lax.Precision.HIGHEST
F32 = jnp.float32
BF16 = jnp.bfloat16


def step_polynomials():
    def axpy(left, weight, right):
        size = max(len(left), len(right))
        left = left + [Fraction(0)] * (size - len(left))
        right = right + [Fraction(0)] * (size - len(right))
        return [a + weight * b for a, b in zip(left, right)]

    inner = [Fraction(1)]
    sections = [[Fraction(0)] + inner]
    for weights in TABLEAU:
        inner = [Fraction(1)]
        for weight, section in zip(weights, sections):
            inner = axpy(inner, Fraction(weight), section)
        sections.append([Fraction(0)] + inner)
    error = [Fraction(0)]
    for weight, section in zip(ERRORS, sections):
        error = axpy(error, Fraction(weight), section)
    return [float(x) for x in inner], [float(x) for x in error]


NEW, ERR = step_polynomials()
POWERS = len(ERR) - 1


def split(x):
    high = x.astype(BF16)
    low = (x - high.astype(F32)).astype(BF16)
    return high, low


def dot(a, b, **kw):
    return jnp.dot(a, b, preferred_element_type=F32, **kw)


def div24(x):
    return lax.shift_right_logical(x * 2731, 16)


def call(body, outs, scratch=(), flops=1000000, name=None, smem=(), args=(), aliases=None):
    specs = [
        pl.BlockSpec(memory_space=pltpu.SMEM if i in smem else pltpu.VMEM) for i in range(len(args))
    ]
    return pl.pallas_call(
        body,
        out_shape=[jax.ShapeDtypeStruct(s, d) for s, d in outs],
        in_specs=specs,
        out_specs=[pl.BlockSpec(memory_space=pltpu.VMEM) for _ in outs],
        scratch_shapes=[pltpu.VMEM(s, d) for s, d in scratch],
        compiler_params=pltpu.CompilerParams(vmem_limit_bytes=24 * 1024 * 1024),
        cost_estimate=pl.CostEstimate(flops=flops, bytes_accessed=4000000, transcendentals=0),
        input_output_aliases=aliases or {},
        name=name,
    )(*args)


def plan_body(src_ref, site_ref, place_ref, piece_ref, ask_ref):
    src = src_ref[...]
    srcf = src.astype(F32)
    turned = jnp.concatenate([srcf, jnp.zeros((LANES - LINKS, LANES), F32)], axis=0).T
    sub = lax.broadcasted_iota(jnp.int32, (LANES, LANES), 0)
    lane = lax.broadcasted_iota(jnp.int32, (LANES, LANES), 1)
    piece_row = lax.broadcasted_iota(jnp.int32, (PIECES, LANES), 0)
    asked = jnp.zeros((LANES, PIECES), F32)
    for l in range(LINKS):
        mine = jnp.broadcast_to(srcf[l : l + 1, :], (LANES, LANES))
        same = jnp.zeros((LANES, LANES), F32)
        for q in range(l + 1):
            other = jnp.broadcast_to(turned[:, q : q + 1], (LANES, LANES))
            hit = other == mine
            if q == l:
                hit = hit & (sub < lane)
            same = same + jnp.where(hit, 1.0, 0.0)
        rank = jnp.sum(same, axis=0, keepdims=True).astype(jnp.int32)
        place = src[l : l + 1, :] - LANES
        slot = lax.bitwise_and(place, SLOT - 1)
        owner = lax.shift_right_arithmetic(place, 1)
        piece = jnp.where(place >= 0, slot * USES + rank, -1)
        piece_ref[l : l + 1, :] = piece
        owned = jnp.where(sub == owner, 1.0, 0.0).astype(BF16)
        place_ref[0:LANES, l * LANES : (l + 1) * LANES] = owned
        place_ref[LANES : 2 * LANES, l * LANES : (l + 1) * LANES] = owned
        wanted = jnp.where(
            piece_row == piece, site_ref[l : l + 1, :].astype(F32), 0.0
        ).astype(BF16)
        asked = asked + lax.dot_general(
            owned, wanted, (((1,), (1,)), ((), ())), preferred_element_type=F32
        )
    ask_ref[...] = jnp.zeros((LANES, LANES), F32)
    ask_ref[:, 0:PIECES] = asked


def tables_body(
    units_ref, ham_ref, rates_ref, modes_ref, coef_ref, send_ref,
    first_ref, second_ref, decay_ref, pick_ref, scaled_ref,
):
    h = units_ref[0].astype(F32) * UNIT_STEP
    ham = ham_ref[...]
    row = lax.broadcasted_iota(jnp.int32, (N, N), 0)
    column = lax.broadcasted_iota(jnp.int32, (N, N), 1)
    unit = jnp.where(row == column, 1.0, 0.0)
    flipped = lax.dot_general(
        unit, ham, (((1,), (1,)), ((), ())), precision=HIGHEST, preferred_element_type=F32
    )
    sym = h * (0.5 * (ham + flipped))
    at = lax.broadcasted_iota(jnp.int32, (N, SQ), 1)
    row = lax.broadcasted_iota(jnp.int32, (N, SQ), 0)
    first = div24(at)
    same_second = row == at - first * N
    by_first = dot(sym, jnp.where(row == first, 1.0, 0.0), precision=HIGHEST)
    by_second = dot(sym, jnp.where(same_second, 1.0, 0.0), precision=HIGHEST)
    first_ref[...] = by_first
    second_ref[...] = by_second
    level = lax.broadcasted_iota(jnp.int32, (rates_ref.shape[1], LANES), 0)
    hits = jnp.zeros((rates_ref.shape[1], LANES), F32)
    for m in range(modes_ref.shape[0]):
        hits = hits + jnp.where(level == modes_ref[m : m + 1, :], 1.0, 0.0)
    rates = jnp.broadcast_to(rates_ref[...], (8, rates_ref.shape[1]))
    decay_ref[...] = h * dot(rates, hits, precision=HIGHEST)
    wide = SLOT * LANES
    i = lax.broadcasted_iota(jnp.int32, (wide, wide), 0)
    p = lax.broadcasted_iota(jnp.int32, (wide, wide), 1)
    order = jnp.where(
        i == lax.bitwise_and(p, LANES - 1) * SLOT + lax.shift_right_logical(p, 7), 1.0, 0.0
    ).astype(BF16)
    ids = jnp.broadcast_to(send_ref[...].astype(F32), (8, wide)).astype(BF16)
    sorted_ids = dot(ids, order)[0:1, :].astype(jnp.int32)
    sub = lax.broadcasted_iota(jnp.int32, (LANES, wide), 0)
    hot = jnp.where(sub == sorted_ids, 1.0, 0.0).astype(BF16)
    pick_ref[0:LANES, :] = hot
    pick_ref[LANES : 2 * LANES, :] = hot
    scaled_ref[...] = h * coef_ref[...]


def lines(read_row, read_column, sites, store):
    for kind, read in ((0, read_row), (1, read_column)):
        kept = [[[None] * 3 for _ in range(2)] for _ in sites]
        for k in range(N):
            tile = [[read(c, k, t) for t in range(3)] for c in range(2)]
            for u, site in enumerate(sites):
                hit = site == k if k else None
                for c in range(2):
                    for t in range(3):
                        kept[u][c][t] = (
                            jnp.where(hit, tile[c][t], kept[u][c][t]) if k else tile[c][t]
                        )
        for u in range(len(sites)):
            for c in range(2):
                for t in range(3):
                    store(u, kind * 2 * N + c * N + t * 8, kept[u][c][t])


def local_part(
    v_ref, first_ref, second_ref, decay_ref, src_ref, site_ref, base, line,
    both_ref, high_ref, low_ref, full,
):
    at = lax.broadcasted_iota(jnp.int32, (N, SQ), 1)
    row = lax.broadcasted_iota(jnp.int32, (N, SQ), 0)
    group = div24(at)
    same_second = row == at - group * N
    by_second = second_ref[...]

    def turns(i, carry):
        parts = []
        for j in range(2):
            a = 2 * i + j
            block = jnp.where(same_second, jnp.broadcast_to(first_ref[pl.ds(a, 1), :], (N, SQ)), 0.0)
            parts.append(block - jnp.where(group == a, by_second, 0.0))
        high, low = split(jnp.concatenate(parts, axis=0))
        rows = pl.ds(pl.multiple_of(i * 2 * N, 2 * N), 2 * N)
        high_ref[rows, :] = high
        low_ref[rows, :] = low
        return carry

    lax.fori_loop(0, N // 2, turns, 0)
    sub = lax.broadcasted_iota(jnp.int32, (LANES, LANES), 0)
    real, imag = v_ref[0:SQ, :], v_ref[SQ:ROWS, :]
    real_high, real_low = split(real)
    imag_high, imag_low = split(imag)
    high = jnp.concatenate([real_high, imag_high], axis=0)
    low = jnp.concatenate([real_low, imag_low], axis=0)
    both_ref[...] = jnp.concatenate([high, low], axis=1)

    def fetch(l, place):
        hot = jnp.where(sub == src_ref[pl.ds(l, 1), :], 1.0, 0.0).astype(BF16)
        place[...] = dot(both_ref[...], jnp.concatenate([hot, hot], axis=0))

    def pick(l, place):
        site = jnp.broadcast_to(site_ref[pl.ds(l, 1), :], (8, LANES))

        def store(u, f, value):
            line[l, f : f + 8, :] = value

        lines(
            lambda c, k, t: place[pl.ds(c * SQ + k * N + t * 8, 8), :],
            lambda c, k, t: place[pl.ds(c * SQ + t * 8 * N + k, 8, stride=N), :],
            [site],
            store,
        )

    def link(l, carry):
        fetch(l, full)
        pick(l, full)
        return carry

    lax.fori_loop(0, LINKS, link, 0)
    x_high = jnp.concatenate([real_high, imag_high], axis=1)
    x_low = jnp.concatenate([real_low, imag_low], axis=1)
    turned = dot(high_ref[...], x_high) + dot(high_ref[...], x_low) + dot(low_ref[...], x_high)
    decay = jnp.broadcast_to(decay_ref[0:1, :], (SQ, LANES))
    base[0:SQ, :] = turned[:, LANES:] - decay * real
    base[SQ:ROWS, :] = -turned[:, :LANES] - decay * imag


def pack_part(v_ref, pick_ref, sites, send_ref, full, feats):
    high, low = split(v_ref[...])
    picked = dot(jnp.concatenate([high, low], axis=1), pick_ref[...])
    for s in range(SLOT):
        full[s] = picked[:, s * LANES : (s + 1) * LANES]
    for s in range(SLOT):
        wanted = [
            jnp.broadcast_to(sites[s * USES + u : s * USES + u + 1, :], (8, LANES))
            for u in range(USES)
        ]

        def store(u, f, value):
            row = (s * USES + u) * LINE + f
            feats[row : row + 8, :] = value

        lines(
            lambda c, k, t: full[s, pl.ds(c * SQ + k * N + t * 8, 8), :],
            lambda c, k, t: full[s, pl.ds(c * SQ + t * 8 * N + k, 8, stride=N), :],
            wanted,
            store,
        )
    for k in range(BLOCKS):
        send_ref[pl.ds(k, LANES, stride=BLOCKS), :] = feats[k * LANES : (k + 1) * LANES, :].T


def first_pack(v, pick, asked):
    def body(v_ref, pick_ref, asked_ref, send_ref, want_ref, full, feats):
        want = asked_ref[...].T[0:PIECES, :].astype(jnp.int32)
        want_ref[...] = want
        pack_part(v_ref, pick_ref, want, send_ref, full, feats)

    return call(
        body,
        [((BLOCKS * LANES, LANES), F32), ((PIECES, LANES), jnp.int32)],
        [((SLOT, ROWS, LANES), F32), ((FEATURES, LANES), F32)],
        flops=10**8, name="pack_first", args=(v, pick, asked),
    )


def gather_part(
    got_ref, place_ref, piece_ref, site_ref, coef_ref, base_ref, line_ref, emit, feats, cols
):
    for k in range(BLOCKS):
        feats[k * LANES : (k + 1) * LANES, :] = got_ref[pl.ds(k, LANES, stride=BLOCKS), :].T
    high, low = split(feats[...])
    wide = jnp.concatenate([high, low], axis=1)
    found = []
    for pair in range(LINKS // 2):
        both = dot(wide, place_ref[:, pair * 2 * LANES : (pair + 1) * 2 * LANES])
        for half in range(2):
            l = pair * 2 + half
            piece = jnp.broadcast_to(piece_ref[l : l + 1, :], (LINE, LANES))
            value = line_ref[l]
            for p in range(PIECES):
                part = both[p * LINE : (p + 1) * LINE, half * LANES : (half + 1) * LANES]
                value = jnp.where(piece == p, part, value)
            found.append(value)
    sites = [jnp.broadcast_to(site_ref[l : l + 1, :], (8, LANES)) for l in range(LINKS)]

    def term(kind, c, l):
        rows = slice(kind * 2 * N, (kind + 1) * 2 * N)
        x = found[l][rows]
        re, im = x[0:N], x[N:]
        row = 2 * kind * LINKS + l
        cr = jnp.broadcast_to(coef_ref[row : row + 1, :], (N, LANES))
        ci = jnp.broadcast_to(coef_ref[row + LINKS : row + LINKS + 1, :], (N, LANES))
        value = cr * im + ci * re if c == 0 else ci * im - cr * re
        return -value if kind else value

    for kind in (1, 0):
        for c in range(2):
            terms = [term(kind, c, l) for l in range(LINKS)]
            for k in range(N):
                hits = [site == k for site in sites]
                for t in range(3):
                    if kind:
                        total = jnp.zeros((8, LANES), F32)
                    else:
                        at = c * SQ + k * N + t * 8
                        total = base_ref[at : at + 8, :]
                        total = total + cols[pl.ds(c * SQ + t * 8 * N + k, 8, stride=N), :]
                    for l in range(LINKS):
                        total = total + jnp.where(hits[l], terms[l][t * 8 : t * 8 + 8], 0.0)
                    if kind:
                        at = c * SQ + k * N + t * 8
                        cols[at : at + 8, :] = total
                    else:
                        emit(at, total)


def local(n, v, total, turn, decay, src, site, last=()):
    add = n > 0

    def body(v_ref, total_ref, first_ref, second_ref, decay_ref, src_ref, site_ref, *refs):
        refs, (both, high, low, full) = refs[:-4], refs[-4:]
        base, line = refs[len(last) : len(last) + 2]
        if add:
            new = total_ref[...] + NEW[n] * v_ref[...]
            refs[len(last) + 2][...] = new
        if last:
            state_ref, before_ref = refs[:2]
            refs[-1][...] = ERR[POWERS] / (
                ABS_TOL + REL_TOL * jnp.maximum(jnp.abs(state_ref[...]), jnp.abs(new))
            )
            error = ERR[POWERS - 2] * before_ref[...] + ERR[POWERS - 1] * v_ref[...]
            both_error = error * (1.0 / ERR[POWERS])
        local_part(
            v_ref, first_ref, second_ref, decay_ref, src_ref, site_ref, base, line,
            both, high, low, full,
        )
        if last:
            base[...] = base[...] + both_error

    return call(
        body,
        [((ROWS, LANES), F32), ((LINKS, LINE, LANES), F32)]
        + [((ROWS, LANES), F32)] * (add + bool(last)),
        [
            ((ROWS, 2 * LANES), BF16),
            ((SQ, SQ), BF16),
            ((SQ, SQ), BF16),
            ((ROWS, LANES), F32),
        ],
        flops=10**9, name="local", args=(v, total, *turn, decay, src, site, *last),
        aliases={1: 2} if 1 < n < POWERS - 1 else {},
    )


def advance(got, base, line, place, piece, pick, coef, site, want):
    def body(got_ref, base_ref, line_ref, place_ref, piece_ref, pick_ref, coef_ref,
             site_ref, want_ref, next_ref, send_ref, full, feats, cols):
        def emit(at, value):
            next_ref[at : at + 8, :] = value

        gather_part(
            got_ref, place_ref, piece_ref, site_ref, coef_ref, base_ref, line_ref, emit, feats, cols
        )
        pack_part(next_ref, pick_ref, want_ref[...], send_ref, full, feats)

    return call(
        body,
        [((ROWS, LANES), F32), ((BLOCKS * LANES, LANES), F32)],
        [((SLOT, ROWS, LANES), F32), ((FEATURES, LANES), F32), ((ROWS, LANES), F32)],
        name="advance", aliases={1: 0},
        args=(got, base, line, place, piece, pick, coef, site, want),
    )


def finish(got, base, line, inverse, place, piece, coef, site):
    def body(got_ref, base_ref, line_ref, inverse_ref, place_ref, piece_ref, coef_ref,
             site_ref, out_ref, feats, cols, sums):
        sums[...] = jnp.zeros((8, LANES), F32)

        def emit(at, value):
            rows = slice(at, at + 8)
            scaled = value * inverse_ref[rows, :]
            sums[...] = sums[...] + scaled * scaled

        gather_part(
            got_ref, place_ref, piece_ref, site_ref, coef_ref, base_ref, line_ref, emit, feats, cols
        )
        out_ref[...] = jnp.broadcast_to(jnp.sum(sums[...], axis=0, keepdims=True), (LANES, LANES))

    (out,) = call(
        body,
        [((LANES, LANES), F32)],
        [((FEATURES, LANES), F32), ((ROWS, LANES), F32), ((8, LANES), F32)],
        name="finish", args=(got, base, line, inverse, place, piece, coef, site),
    )
    return out


def exchange(x):
    peers = LANES
    flat = x.reshape(peers, 1, x.size // peers)
    moved = lax.all_to_all(flat, ALL, split_axis=0, concat_axis=0, tiled=True)
    return moved.reshape(x.shape)


def shards(
    state, hamiltonian, mode_rates, ado_modes, link_src, link_site, link_coef, send_ids, step_units
):
    v = state.reshape(ROWS, LANES)
    place, piece, ask = call(
        plan_body,
        [((2 * LANES, COUPLINGS), BF16), ((LINKS, LANES), jnp.int32), ((LANES, LANES), F32)],
        flops=10**8, name="plan", args=(link_src, link_site),
    )
    asked = exchange(ask)
    *turn, decay, pick, coef = call(
        tables_body,
        [
            ((N, SQ), F32),
            ((N, SQ), F32),
            ((8, LANES), F32),
            ((2 * LANES, SLOT * LANES), BF16),
            ((4 * LINKS, LANES), F32),
        ],
        flops=10**9, name="tables", smem=(0,),
        args=(
            step_units.reshape(1), hamiltonian, mode_rates.reshape(1, -1), ado_modes,
            link_coef.reshape(4 * LINKS, LANES), send_ids,
        ),
    )
    send, want = first_pack(v, pick, asked)
    total = v
    for n in range(POWERS - 1):
        got = exchange(send)
        base, line, *added = local(n, v, total, turn, decay, link_src, link_site)
        if added:
            (total,) = added
        before = v
        v, send = advance(got, base, line, place, piece, pick, coef, link_site, want)
    got = exchange(send)
    start = lax.optimization_barrier((state, v))[0].reshape(ROWS, LANES)
    base, line, total, inverse = local(
        POWERS - 1, v, total, turn, decay, link_src, link_site, (start, before)
    )
    sums = exchange(finish(got, base, line, inverse, place, piece, coef, link_site))
    entries = state.size * lax.axis_size(ALL)
    return total.reshape(state.shape), jnp.sqrt(jnp.sum(sums) / entries)


def solution(mesh):
    return jax.shard_map(
        shards,
        mesh=mesh,
        in_specs=(
            P(None, None, None, ALL),
            P(),
            P(),
            P(None, ALL),
            P(None, ALL),
            P(None, ALL),
            P(None, None, ALL),
            P(ALL, None),
            P(),
        ),
        out_specs=(P(None, None, None, ALL), P()),
        check_vma=False,
    )
```

```python
from fractions import Fraction

import jax
import jax.numpy as jnp
from jax import lax
from jax.experimental import pallas as pl
from jax.experimental.pallas import tpu as pltpu
from jax.sharding import PartitionSpec as P

ALL = ("grp", "dev")

TABLEAU = (
    ("1/5",),
    ("3/40", "9/40"),
    ("44/45", "-56/15", "32/9"),
    ("19372/6561", "-25360/2187", "64448/6561", "-212/729"),
    ("9017/3168", "-355/33", "46732/5247", "49/176", "-5103/18656"),
    ("35/384", "0", "500/1113", "125/192", "-2187/6784", "11/84"),
)
ERRORS = ("71/57600", "0", "-71/16695", "71/1920", "-17253/339200", "22/525", "-1/40")
ABS_TOL = 0.001
REL_TOL = 0.01
UNIT_STEP = 1.0 / 64

N = 24
LINKS = 8
SLOT = 2
USES = 4
LANES = 128
SQ = N * N
ROWS = 2 * SQ
LINE = 4 * N
PIECES = SLOT * USES
FEATURES = PIECES * LINE
BLOCKS = FEATURES // LANES
COUPLINGS = LINKS * LANES
HIGHEST = lax.Precision.HIGHEST
F32 = jnp.float32
BF16 = jnp.bfloat16


def step_polynomials():
    def axpy(left, weight, right):
        size = max(len(left), len(right))
        left = left + [Fraction(0)] * (size - len(left))
        right = right + [Fraction(0)] * (size - len(right))
        return [a + weight * b for a, b in zip(left, right)]

    inner = [Fraction(1)]
    sections = [[Fraction(0)] + inner]
    for weights in TABLEAU:
        inner = [Fraction(1)]
        for weight, section in zip(weights, sections):
            inner = axpy(inner, Fraction(weight), section)
        sections.append([Fraction(0)] + inner)
    error = [Fraction(0)]
    for weight, section in zip(ERRORS, sections):
        error = axpy(error, Fraction(weight), section)
    return [float(x) for x in inner], [float(x) for x in error]


NEW, ERR = step_polynomials()
POWERS = len(ERR) - 1


def split(x):
    high = x.astype(BF16)
    low = (x - high.astype(F32)).astype(BF16)
    return high, low


def dot(a, b, **kw):
    return jnp.dot(a, b, preferred_element_type=F32, **kw)


def div24(x):
    return lax.shift_right_logical(x * 2731, 16)


def call(body, outs, scratch=(), flops=1000000, name=None, smem=(), args=(), aliases=None):
    specs = [
        pl.BlockSpec(memory_space=pltpu.SMEM if i in smem else pltpu.VMEM) for i in range(len(args))
    ]
    return pl.pallas_call(
        body,
        out_shape=[jax.ShapeDtypeStruct(s, d) for s, d in outs],
        in_specs=specs,
        out_specs=[pl.BlockSpec(memory_space=pltpu.VMEM) for _ in outs],
        scratch_shapes=[pltpu.VMEM(s, d) for s, d in scratch],
        compiler_params=pltpu.CompilerParams(vmem_limit_bytes=24 * 1024 * 1024),
        cost_estimate=pl.CostEstimate(flops=flops, bytes_accessed=4000000, transcendentals=0),
        input_output_aliases=aliases or {},
        name=name,
    )(*args)


def plan_body(src_ref, site_ref, place_ref, piece_ref, ask_ref):
    src = src_ref[...]
    srcf = src.astype(F32)
    turned = jnp.concatenate([srcf, jnp.zeros((LANES - LINKS, LANES), F32)], axis=0).T
    sub = lax.broadcasted_iota(jnp.int32, (LANES, LANES), 0)
    lane = lax.broadcasted_iota(jnp.int32, (LANES, LANES), 1)
    piece_row = lax.broadcasted_iota(jnp.int32, (PIECES, LANES), 0)
    asked = jnp.zeros((LANES, PIECES), F32)
    for l in range(LINKS):
        mine = jnp.broadcast_to(srcf[l : l + 1, :], (LANES, LANES))
        same = jnp.zeros((LANES, LANES), F32)
        for q in range(l + 1):
            other = jnp.broadcast_to(turned[:, q : q + 1], (LANES, LANES))
            hit = other == mine
            if q == l:
                hit = hit & (sub < lane)
            same = same + jnp.where(hit, 1.0, 0.0)
        rank = jnp.sum(same, axis=0, keepdims=True).astype(jnp.int32)
        place = src[l : l + 1, :] - LANES
        slot = lax.bitwise_and(place, SLOT - 1)
        owner = lax.shift_right_arithmetic(place, 1)
        piece = jnp.where(place >= 0, slot * USES + rank, -1)
        piece_ref[l : l + 1, :] = piece
        owned = jnp.where(sub == owner, 1.0, 0.0).astype(BF16)
        place_ref[0:LANES, l * LANES : (l + 1) * LANES] = owned
        place_ref[LANES : 2 * LANES, l * LANES : (l + 1) * LANES] = owned
        wanted = jnp.where(
            piece_row == piece, site_ref[l : l + 1, :].astype(F32), 0.0
        ).astype(BF16)
        asked = asked + lax.dot_general(
            owned, wanted, (((1,), (1,)), ((), ())), preferred_element_type=F32
        )
    ask_ref[...] = jnp.zeros((LANES, LANES), F32)
    ask_ref[:, 0:PIECES] = asked


def tables_body(
    units_ref, ham_ref, rates_ref, modes_ref, coef_ref, send_ref,
    first_ref, second_ref, decay_ref, pick_ref, scaled_ref,
):
    h = units_ref[0].astype(F32) * UNIT_STEP
    ham = ham_ref[...]
    row = lax.broadcasted_iota(jnp.int32, (N, N), 0)
    column = lax.broadcasted_iota(jnp.int32, (N, N), 1)
    unit = jnp.where(row == column, 1.0, 0.0)
    flipped = lax.dot_general(
        unit, ham, (((1,), (1,)), ((), ())), precision=HIGHEST, preferred_element_type=F32
    )
    sym = h * (0.5 * (ham + flipped))
    at = lax.broadcasted_iota(jnp.int32, (N, SQ), 1)
    row = lax.broadcasted_iota(jnp.int32, (N, SQ), 0)
    first = div24(at)
    same_second = row == at - first * N
    by_first = dot(sym, jnp.where(row == first, 1.0, 0.0), precision=HIGHEST)
    by_second = dot(sym, jnp.where(same_second, 1.0, 0.0), precision=HIGHEST)
    first_ref[...] = by_first
    second_ref[...] = by_second
    level = lax.broadcasted_iota(jnp.int32, (rates_ref.shape[1], LANES), 0)
    hits = jnp.zeros((rates_ref.shape[1], LANES), F32)
    for m in range(modes_ref.shape[0]):
        hits = hits + jnp.where(level == modes_ref[m : m + 1, :], 1.0, 0.0)
    rates = jnp.broadcast_to(rates_ref[...], (8, rates_ref.shape[1]))
    decay_ref[...] = h * dot(rates, hits, precision=HIGHEST)
    wide = SLOT * LANES
    i = lax.broadcasted_iota(jnp.int32, (wide, wide), 0)
    p = lax.broadcasted_iota(jnp.int32, (wide, wide), 1)
    order = jnp.where(
        i == lax.bitwise_and(p, LANES - 1) * SLOT + lax.shift_right_logical(p, 7), 1.0, 0.0
    ).astype(BF16)
    ids = jnp.broadcast_to(send_ref[...].astype(F32), (8, wide)).astype(BF16)
    sorted_ids = dot(ids, order)[0:1, :].astype(jnp.int32)
    sub = lax.broadcasted_iota(jnp.int32, (LANES, wide), 0)
    hot = jnp.where(sub == sorted_ids, 1.0, 0.0).astype(BF16)
    pick_ref[0:LANES, :] = hot
    pick_ref[LANES : 2 * LANES, :] = hot
    scaled_ref[...] = h * coef_ref[...]


def lines(read_row, read_column, sites, store):
    for kind, read in ((0, read_row), (1, read_column)):
        kept = [[[None] * 3 for _ in range(2)] for _ in sites]
        for k in range(N):
            tile = [[read(c, k, t) for t in range(3)] for c in range(2)]
            for u, site in enumerate(sites):
                hit = site == k if k else None
                for c in range(2):
                    for t in range(3):
                        kept[u][c][t] = (
                            jnp.where(hit, tile[c][t], kept[u][c][t]) if k else tile[c][t]
                        )
        for u in range(len(sites)):
            for c in range(2):
                for t in range(3):
                    store(u, kind * 2 * N + c * N + t * 8, kept[u][c][t])


def local_part(
    v_ref, first_ref, second_ref, decay_ref, src_ref, site_ref, base, line,
    both_ref, high_ref, low_ref, full,
):
    at = lax.broadcasted_iota(jnp.int32, (N, SQ), 1)
    row = lax.broadcasted_iota(jnp.int32, (N, SQ), 0)
    group = div24(at)
    same_second = row == at - group * N
    by_second = second_ref[...]

    def turns(i, carry):
        parts = []
        for j in range(2):
            a = 2 * i + j
            block = jnp.where(same_second, jnp.broadcast_to(first_ref[pl.ds(a, 1), :], (N, SQ)), 0.0)
            parts.append(block - jnp.where(group == a, by_second, 0.0))
        high, low = split(jnp.concatenate(parts, axis=0))
        rows = pl.ds(pl.multiple_of(i * 2 * N, 2 * N), 2 * N)
        high_ref[rows, :] = high
        low_ref[rows, :] = low
        return carry

    lax.fori_loop(0, N // 2, turns, 0)
    sub = lax.broadcasted_iota(jnp.int32, (LANES, LANES), 0)
    real, imag = v_ref[0:SQ, :], v_ref[SQ:ROWS, :]
    real_high, real_low = split(real)
    imag_high, imag_low = split(imag)
    high = jnp.concatenate([real_high, imag_high], axis=0)
    low = jnp.concatenate([real_low, imag_low], axis=0)
    both_ref[...] = jnp.concatenate([high, low], axis=1)

    def fetch(l, place):
        hot = jnp.where(sub == src_ref[pl.ds(l, 1), :], 1.0, 0.0).astype(BF16)
        place[...] = dot(both_ref[...], jnp.concatenate([hot, hot], axis=0))

    def pick(l, place):
        site = jnp.broadcast_to(site_ref[pl.ds(l, 1), :], (8, LANES))

        def store(u, f, value):
            line[l, f : f + 8, :] = value

        lines(
            lambda c, k, t: place[pl.ds(c * SQ + k * N + t * 8, 8), :],
            lambda c, k, t: place[pl.ds(c * SQ + t * 8 * N + k, 8, stride=N), :],
            [site],
            store,
        )

    def link(l, carry):
        fetch(l, full)
        pick(l, full)
        return carry

    lax.fori_loop(0, LINKS, link, 0)
    chunk = SQ // 3
    decay = jnp.broadcast_to(decay_ref[0:1, :], (chunk, LANES))

    def commute(i, carry):
        rows = pl.ds(pl.multiple_of(i * chunk, chunk), chunk)
        after = pl.ds(pl.multiple_of(SQ + i * chunk, chunk), chunk)
        x_high, x_low = (
            jnp.concatenate([both_ref[0:SQ, half], both_ref[SQ:ROWS, half]], axis=1)
            for half in (slice(0, LANES), slice(LANES, 2 * LANES))
        )
        turned = (
            dot(high_ref[rows, :], x_high) + dot(high_ref[rows, :], x_low) + dot(low_ref[rows, :], x_high)
        )
        base[rows, :] = turned[:, LANES:] - decay * v_ref[rows, :]
        base[after, :] = -turned[:, :LANES] - decay * v_ref[after, :]
        return carry

    lax.fori_loop(0, 3, commute, 0)


def pack_part(v_ref, pick_ref, sites, send_ref, full, feats):
    high, low = split(v_ref[...])
    picked = dot(jnp.concatenate([high, low], axis=1), pick_ref[...])
    for s in range(SLOT):
        full[s] = picked[:, s * LANES : (s + 1) * LANES]
    for s in range(SLOT):
        wanted = [
            jnp.broadcast_to(sites[s * USES + u : s * USES + u + 1, :], (8, LANES))
            for u in range(USES)
        ]

        def store(u, f, value):
            row = (s * USES + u) * LINE + f
            feats[row : row + 8, :] = value

        lines(
            lambda c, k, t: full[s, pl.ds(c * SQ + k * N + t * 8, 8), :],
            lambda c, k, t: full[s, pl.ds(c * SQ + t * 8 * N + k, 8, stride=N), :],
            wanted,
            store,
        )
    for k in range(BLOCKS):
        send_ref[pl.ds(k, LANES, stride=BLOCKS), :] = feats[k * LANES : (k + 1) * LANES, :].T


def first_pack(v, pick, asked):
    def body(v_ref, pick_ref, asked_ref, send_ref, want_ref, full, feats):
        want = asked_ref[...].T[0:PIECES, :].astype(jnp.int32)
        want_ref[...] = want
        pack_part(v_ref, pick_ref, want, send_ref, full, feats)

    return call(
        body,
        [((BLOCKS * LANES, LANES), F32), ((PIECES, LANES), jnp.int32)],
        [((SLOT, ROWS, LANES), F32), ((FEATURES, LANES), F32)],
        flops=10**8, name="pack_first", args=(v, pick, asked),
    )


def gather_part(
    got_ref, place_ref, piece_ref, site_ref, coef_ref, base_ref, line_ref, emit, feats, cols
):
    for k in range(BLOCKS):
        feats[k * LANES : (k + 1) * LANES, :] = got_ref[pl.ds(k, LANES, stride=BLOCKS), :].T
    high, low = split(feats[...])
    wide = jnp.concatenate([high, low], axis=1)
    found = []
    for pair in range(LINKS // 2):
        both = dot(wide, place_ref[:, pair * 2 * LANES : (pair + 1) * 2 * LANES])
        for half in range(2):
            l = pair * 2 + half
            piece = jnp.broadcast_to(piece_ref[l : l + 1, :], (8, LANES))
            if line_ref is None:
                tiles = [jnp.zeros((8, LANES), F32)] * (LINE // 8)
            else:
                tiles = [line_ref[l, f : f + 8, :] for f in range(0, LINE, 8)]
            for p in range(PIECES):
                hit = piece == p
                for t in range(LINE // 8):
                    f = p * LINE + t * 8
                    part = both[f : f + 8, half * LANES : (half + 1) * LANES]
                    tiles[t] = jnp.where(hit, part, tiles[t])
            found.append(jnp.concatenate(tiles, axis=0))
    scatter_part(found, site_ref, coef_ref, base_ref, emit, cols)


def scatter_part(found, site_ref, coef_ref, base_ref, emit, cols):
    sites = [jnp.broadcast_to(site_ref[l : l + 1, :], (8, LANES)) for l in range(LINKS)]

    def term(kind, c, l):
        rows = slice(kind * 2 * N, (kind + 1) * 2 * N)
        x = found[l][rows]
        re, im = x[0:N], x[N:]
        row = 2 * kind * LINKS + l
        cr = jnp.broadcast_to(coef_ref[row : row + 1, :], (N, LANES))
        ci = jnp.broadcast_to(coef_ref[row + LINKS : row + LINKS + 1, :], (N, LANES))
        value = cr * im + ci * re if c == 0 else ci * im - cr * re
        return -value if kind else value

    for kind in (1, 0):
        for c in range(2):
            terms = [term(kind, c, l) for l in range(LINKS)]
            for k in range(N):
                hits = [site == k for site in sites]
                for t in range(3):
                    if kind:
                        total = None
                    else:
                        at = c * SQ + k * N + t * 8
                        total = base_ref[at : at + 8, :]
                        total = total + cols[pl.ds(c * SQ + t * 8 * N + k, 8, stride=N), :]
                    for l in range(LINKS):
                        part = jnp.where(hits[l], terms[l][t * 8 : t * 8 + 8], 0.0)
                        total = part if total is None else total + part
                    if kind:
                        at = c * SQ + k * N + t * 8
                        cols[at : at + 8, :] = total
                    else:
                        emit(at, total)


def local(n, v, total, turn, decay, src, site, last=()):
    add = n > 0

    def body(v_ref, total_ref, first_ref, second_ref, decay_ref, src_ref, site_ref, *refs):
        inputs, refs = refs[: len(last)], refs[len(last) :]
        if last:
            state_ref, before_ref, coef_ref = inputs
            base, sum_ref, inverse_ref, both, high, low, full, kept, line, cols = refs
        elif add:
            base, line, sum_ref, both, high, low, full = refs
        else:
            base, line, both, high, low, full = refs
        if add:
            sum_ref[...] = total_ref[...] + NEW[n] * v_ref[...]
        if last:
            inverse_ref[...] = ERR[POWERS] / (
                ABS_TOL + REL_TOL * jnp.maximum(jnp.abs(state_ref[...]), jnp.abs(sum_ref[...]))
            )
            error = ERR[POWERS - 2] * before_ref[...] + ERR[POWERS - 1] * v_ref[...]
            kept[...] = error * (1.0 / ERR[POWERS])
        local_part(
            v_ref, first_ref, second_ref, decay_ref, src_ref, site_ref,
            full if last else base, line, both, high, low, full,
        )
        if last:
            kept[...] = kept[...] + full[...]

            def emit(at, value):
                base[at : at + 8, :] = value

            found = [line[l] for l in range(LINKS)]
            scatter_part(found, site_ref, coef_ref, kept, emit, cols)

    square = ((ROWS, LANES), F32)
    lines_of_links = ((LINKS, LINE, LANES), F32)
    return call(
        body,
        [square] * 3 if last else [square, lines_of_links] + [square] * add,
        [((ROWS, 2 * LANES), BF16), ((SQ, SQ), BF16), ((SQ, SQ), BF16), square]
        + ([square, lines_of_links, square] if last else []),
        flops=10**9, name="local", args=(v, total, *turn, decay, src, site, *last),
        aliases={1: 1} if last else {1: 2} if n > 1 else {},
    )


def advance(got, base, line, place, piece, pick, coef, site, want):
    def body(got_ref, base_ref, line_ref, place_ref, piece_ref, pick_ref, coef_ref,
             site_ref, want_ref, next_ref, send_ref, full, feats, cols):
        def emit(at, value):
            next_ref[at : at + 8, :] = value

        gather_part(
            got_ref, place_ref, piece_ref, site_ref, coef_ref, base_ref, line_ref, emit, feats, cols
        )
        pack_part(next_ref, pick_ref, want_ref[...], send_ref, full, feats)

    return call(
        body,
        [((ROWS, LANES), F32), ((BLOCKS * LANES, LANES), F32)],
        [((SLOT, ROWS, LANES), F32), ((FEATURES, LANES), F32), ((ROWS, LANES), F32)],
        name="advance", aliases={1: 0},
        args=(got, base, line, place, piece, pick, coef, site, want),
    )


def finish(got, base, inverse, place, piece, coef, site):
    def body(got_ref, base_ref, inverse_ref, place_ref, piece_ref, coef_ref,
             site_ref, out_ref, feats, cols, sums):
        sums[...] = jnp.zeros((8, LANES), F32)

        def emit(at, value):
            rows = slice(at, at + 8)
            scaled = value * inverse_ref[rows, :]
            sums[...] = sums[...] + scaled * scaled

        gather_part(
            got_ref, place_ref, piece_ref, site_ref, coef_ref, base_ref, None, emit, feats, cols
        )
        out_ref[...] = jnp.broadcast_to(jnp.sum(sums[...], axis=0, keepdims=True), (LANES, LANES))

    (out,) = call(
        body,
        [((LANES, LANES), F32)],
        [((FEATURES, LANES), F32), ((ROWS, LANES), F32), ((8, LANES), F32)],
        name="finish", args=(got, base, inverse, place, piece, coef, site),
    )
    return out


def exchange(x):
    peers = LANES
    flat = x.reshape(peers, 1, x.size // peers)
    moved = lax.all_to_all(flat, ALL, split_axis=0, concat_axis=0, tiled=True)
    return moved.reshape(x.shape)


def shards(
    state, hamiltonian, mode_rates, ado_modes, link_src, link_site, link_coef, send_ids, step_units
):
    v = state.reshape(ROWS, LANES)
    place, piece, ask = call(
        plan_body,
        [((2 * LANES, COUPLINGS), BF16), ((LINKS, LANES), jnp.int32), ((LANES, LANES), F32)],
        flops=10**8, name="plan", args=(link_src, link_site),
    )
    asked = exchange(ask)
    *turn, decay, pick, coef = call(
        tables_body,
        [
            ((N, SQ), F32),
            ((N, SQ), F32),
            ((8, LANES), F32),
            ((2 * LANES, SLOT * LANES), BF16),
            ((4 * LINKS, LANES), F32),
        ],
        flops=10**9, name="tables", smem=(0,),
        args=(
            step_units.reshape(1), hamiltonian, mode_rates.reshape(1, -1), ado_modes,
            link_coef.reshape(4 * LINKS, LANES), send_ids,
        ),
    )
    send, want = first_pack(v, pick, asked)
    total = v
    for n in range(POWERS - 1):
        got = exchange(send)
        base, line, *added = local(n, v, total, turn, decay, link_src, link_site)
        if added:
            (total,) = added
        before = v
        v, send = advance(got, base, line, place, piece, pick, coef, link_site, want)
    got = exchange(send)
    start = lax.optimization_barrier((state, v))[0].reshape(ROWS, LANES)
    base, total, inverse = local(
        POWERS - 1, v, total, turn, decay, link_src, link_site, (start, before, coef)
    )
    sums = exchange(finish(got, base, inverse, place, piece, coef, link_site))
    entries = state.size * lax.axis_size(ALL)
    return total.reshape(state.shape), jnp.sqrt(jnp.sum(sums) / entries)


def solution(mesh):
    return jax.shard_map(
        shards,
        mesh=mesh,
        in_specs=(
            P(None, None, None, ALL),
            P(),
            P(),
            P(None, ALL),
            P(None, ALL),
            P(None, ALL),
            P(None, None, ALL),
            P(ALL, None),
            P(),
        ),
        out_specs=(P(None, None, None, ALL), P()),
        check_vma=False,
    )
```
